32 devices in a mesh: grp: 4 (over z), dev: 8 (over y, x, core).
Axes of the slice: x: 2, y: 2, z: 4, core: 2. Of those that a mesh axis runs over, the one named last changes fastest.
Arguments:
- blocks: bfloat16 [4096, 128, 128], P(('grp', 'dev')), may hold values from -0.29882812 to 0.29882812
- ids_one: int32 [2, 4096], P(None, ('grp', 'dev')), may hold values from 0 to 255, as said below
- ids_two: int32 [2, 2048], P(None, ('grp', 'dev')), may hold values from 0 to 127, as said below
- ids_three: int32 [2, 1024], P(None, ('grp', 'dev')), may hold values from 0 to 63
- match_one: int32 [256, 128], replicated, may hold values from 0 to 127, as said below
- match_two: int32 [128, 128], replicated, may hold values from 0 to 127, as said below
- match_three: int32 [64, 128], replicated, may hold values from 0 to 127, as said below
- target_one: int32 [4096], P(('grp', 'dev')), may hold values from 0 to 63
- target_two: int32 [2048], P(('grp', 'dev')), may hold values from 0 to 31
- target_three: int32 [1024], P(('grp', 'dev')), may hold values from 0 to 15
- vertex_weights: float32 [256, 128], P(('grp', 'dev')), may hold values from 0.1 to 120, as said below
Outputs:
- coarse_graph: float32 [512, 128, 128], P(('grp', 'dev'))
- rel_weight: float32 [32, 128], P(('grp', 'dev'))
The draws below stay inside these ranges and needn't reach their ends.
Inputs may be any that keep to these rules, and one draw needn't show every extreme that they name: `match_one`: rows 2b and 2b + 1 together name every number 0 to 127 exactly twice. `match_two`: rows 2b and 2b + 1 together name every number 0 to 127 exactly twice. `match_three`: rows 2b and 2b + 1 together name every number 0 to 127 exactly twice. `ids_one`: a fine block's row and column vertex blocks, halved by integer division, are the ids_two of the coarse slot it goes to. `ids_two`: a first-level block's row and column vertex blocks, halved by integer division, are the ids_three of the coarse slot it goes to. `vertex_weights`: positive.
All inputs are finite; a program needn't handle non-finite values.
Results may differ from the reference program's by a relative error of at most 0.0003.
Values may be sent and summed in bfloat16 or wider, within the bound.
No kernel may reach another device: no remote copies, remote signals or barrier semaphores. Data moves between devices by JAX's collectives and lax.ppermute only.
A program may use at most 128 MiB of HBM per device.

```python
import math
import jax
import jax.numpy as jnp
from jax import lax

BLOCK = 128
SLOTS = 128
VWB = 8
NFINE = 4096
N_GRP = 4
N_DEV = 8
DEVICES = 32


def pairing(key, count):
    keys = jax.random.split(key, count // 2)
    perms = jax.vmap(lambda single: jax.random.permutation(single, 2 * BLOCK))(keys)
    return (perms // 2).reshape(count, BLOCK).astype(jnp.int32)


def route(count, per_dev, targets):
    slot = jnp.arange(count, dtype=jnp.int32)
    device = slot // per_dev
    local = slot % per_dev
    owner = device // N_DEV * N_DEV + local // (per_dev // N_DEV)
    return (owner * (per_dev // 2) + targets).astype(jnp.int32)


def layout(key):
    keys = jax.random.split(jax.random.fold_in(key, 7), 6)
    nfine = SLOTS * DEVICES
    vbzero = VWB * DEVICES
    ids_three = jax.random.randint(keys[0], (2, nfine // 4), 0, vbzero // 4, dtype=jnp.int32)
    target_two = jax.random.randint(keys[1], (nfine // 2,), 0, SLOTS // 4, dtype=jnp.int32)
    dest_two = route(nfine // 2, SLOTS // 2, target_two)
    ids_two = 2 * ids_three[:, dest_two] + jax.random.randint(keys[2], (2, nfine // 2), 0, 2, dtype=jnp.int32)
    target_one = jax.random.randint(keys[3], (nfine,), 0, SLOTS // 2, dtype=jnp.int32)
    dest_one = route(nfine, SLOTS, target_one)
    ids_one = 2 * ids_two[:, dest_one] + jax.random.randint(keys[4], (2, nfine), 0, 2, dtype=jnp.int32)
    target_three = jax.random.randint(keys[5], (nfine // 4,), 0, SLOTS // 8, dtype=jnp.int32)
    return (ids_one.astype(jnp.int32), ids_two.astype(jnp.int32), ids_three.astype(jnp.int32), target_one, target_two, target_three)


def draw_ids_one(key, part):
    return layout(key)[0]


def draw_ids_two(key, part):
    return layout(key)[1]


def draw_ids_three(key, part):
    return layout(key)[2]


def draw_target_one(key, part):
    return layout(key)[3]


def draw_target_two(key, part):
    return layout(key)[4]


def draw_target_three(key, part):
    return layout(key)[5]


def draw_match_one(key, part):
    return pairing(jax.random.fold_in(key, 11), VWB * DEVICES)


def draw_match_two(key, part):
    return pairing(jax.random.fold_in(key, 12), VWB * DEVICES // 2)


def draw_match_three(key, part):
    return pairing(jax.random.fold_in(key, 13), VWB * DEVICES // 4)


def draw_vertex_weights(key, part):
    first, second = jax.random.split(jax.random.fold_in(key, 21))
    count = VWB * DEVICES
    scale = jnp.exp(jax.random.uniform(first, (count, 1), jnp.float32, 0.0, math.log(16.0)))
    values = jax.random.uniform(second, (count, BLOCK), jnp.float32, 0.5, 1.5)
    return (scale * values).astype(jnp.float32)


def block_levels(own_key, extent, cuts, least, high):
    level = 1.0
    for position, shards_of in cuts:
        draws = jax.random.uniform(jax.random.fold_in(jax.random.fold_in(own_key, 6), position), (shards_of,), jnp.float32, least / len(cuts), high / len(cuts))
        level = level * jnp.repeat(jnp.exp(draws), extent[position] // shards_of).reshape((-1,) + (1,) * (len(extent) - 1 - position))
    return level


def scatter_about(own_key, dims, spread, reach, shards=(), kind=jnp.bfloat16):
    array = jax.random.normal(own_key, dims, jnp.float32) * spread
    if len(shards) > 0:
        array = block_levels(own_key, dims, shards, -0.22, 0.18) * array
    return jnp.clip(array, min=-reach, max=reach).astype(kind)


def setup_inputs(seed: int = 0) -> dict:
    key_list = jax.random.split(jax.random.key(seed), 12)
    return {
        "blocks": scatter_about(key_list[0], (NFINE, BLOCK, BLOCK), 0.05, 0.29882812, ((0, 32),)),
        "ids_one": draw_ids_one(jax.random.fold_in(key_list[11], 71), 0),
        "ids_two": draw_ids_two(jax.random.fold_in(key_list[11], 71), 0),
        "ids_three": draw_ids_three(jax.random.fold_in(key_list[11], 71), 0),
        "match_one": draw_match_one(jax.random.fold_in(key_list[11], 71), 0),
        "match_two": draw_match_two(jax.random.fold_in(key_list[11], 71), 0),
        "match_three": draw_match_three(jax.random.fold_in(key_list[11], 71), 0),
        "target_one": draw_target_one(jax.random.fold_in(key_list[11], 71), 0),
        "target_two": draw_target_two(jax.random.fold_in(key_list[11], 71), 0),
        "target_three": draw_target_three(jax.random.fold_in(key_list[11], 71), 0),
        "vertex_weights": draw_vertex_weights(jax.random.fold_in(key_list[11], 71), 0),
    }


def project_blocks(blocks, pair_ids, table):
    row_map = table[pair_ids[0]]
    col_map = table[pair_ids[1]]

    def single(matrix, rows, cols):
        halfway = jax.ops.segment_sum(matrix.astype(jnp.float32), rows, num_segments=BLOCK)
        return jax.ops.segment_sum(halfway.T, cols, num_segments=BLOCK).T

    return jax.vmap(single)(blocks, row_map, col_map)


def coarsen(blocks, pair_ids, table, targets, per_dev, fold_groups):
    count = blocks.shape[0]
    slot = jnp.arange(count, dtype=jnp.int32)
    device = slot // per_dev
    local = slot % per_dev
    group = device // N_DEV
    member = device % N_DEV
    if fold_groups:
        owner = (local // (per_dev // N_GRP)) * N_DEV + member
    else:
        owner = group * N_DEV + local // (per_dev // N_DEV)
    dest = (owner * (per_dev // 2) + targets).astype(jnp.int32)
    width = math.gcd(count, 512)
    turns = count // width
    inputs = (blocks.reshape(turns, width, BLOCK, BLOCK),
              pair_ids.reshape(2, turns, width).transpose(1, 0, 2),
              dest.reshape(turns, width))

    def accumulate(total, piece):
        part = project_blocks(piece[0], piece[1], table)
        return total.at[piece[2]].add(part), None

    start = jnp.zeros((count // 2, BLOCK, BLOCK), jnp.float32)
    coarse, _ = lax.scan(accumulate, start, inputs)
    return coarse


def pair_weights(weights, table):
    count = weights.shape[0]
    index = (jnp.arange(count, dtype=jnp.int32)[:, None] // 2) * BLOCK + table.astype(jnp.int32)
    summed = jax.ops.segment_sum(weights.reshape(-1), index.reshape(-1), num_segments=count // 2 * BLOCK)
    return summed.reshape(count // 2, BLOCK)


def reference(blocks, ids_one, ids_two, ids_three, match_one, match_two, match_three, target_one, target_two, target_three, vertex_weights):
    coarse_one = coarsen(blocks, ids_one, match_one, target_one, SLOTS, False)
    coarse_two = coarsen(coarse_one, ids_two, match_two, target_two, SLOTS // 2, False)
    coarse_graph = coarsen(coarse_two, ids_three, match_three, target_three, SLOTS // 4, True)
    weights_three = pair_weights(pair_weights(pair_weights(vertex_weights, match_one), match_two), match_three)
    total = jnp.sum(vertex_weights)
    rel_weight = weights_three * (weights_three.shape[0] * BLOCK) / total
    return coarse_graph, rel_weight
```

```python
import functools

import jax
import jax.numpy as jnp
from jax import lax
from jax.experimental import pallas as pl
from jax.experimental.pallas import tpu as pltpu
from jax.sharding import PartitionSpec as P

LEVELS = 32766.0
STEP = 16.0
FINE_STEPS = 8
HALVES = 2


def up(count, unit):
    return -(-count // unit) * unit


def one_hot(indices, width):
    rows = lax.broadcasted_iota(jnp.int32, (width, indices.shape[1]), 0)
    return jnp.where(rows == indices, 1.0, 0.0).astype(jnp.bfloat16)


def contract_lanes(left, right):
    return lax.dot_general(
        left, right, (((1,), (1,)), ((), ())), preferred_element_type=jnp.float32
    )


def compose_kernel(one_ref, two_ref, three_ref, own_ref, weights_ref, table_ref, coarse_ref):
    middle = jnp.take_along_axis(two_ref[...], one_ref[...], axis=1)
    table_ref[...] = jnp.take_along_axis(three_ref[...], middle, axis=1)
    owned, width = weights_ref.shape
    total = jnp.zeros((8, width), jnp.float32)
    for row in range(owned):
        hot = one_hot(table_ref[pl.ds(own_ref[0] + row, 1), :], width)
        value = weights_ref[row : row + 1, :]
        high = value.astype(jnp.bfloat16)
        rest = value - high.astype(jnp.float32)
        middle_part = rest.astype(jnp.bfloat16)
        low = (rest - middle_part.astype(jnp.float32)).astype(jnp.bfloat16)
        parts = jnp.concatenate(
            [high.astype(jnp.float32), middle_part.astype(jnp.float32), low.astype(jnp.float32),
             jnp.zeros((5, width), jnp.float32)], axis=0).astype(jnp.bfloat16)
        total = total + contract_lanes(parts, hot)
    coarse_ref[...] = jnp.sum(total, axis=0, keepdims=True)


def compose(match_one, match_two, match_three, weights, position):
    count, width = match_one.shape
    two = jnp.repeat(match_two, 2, axis=0)
    three = jnp.repeat(match_three, 4, axis=0)
    own = (position * weights.shape[0]).astype(jnp.int32).reshape(1)
    vmem = pl.BlockSpec(memory_space=pltpu.VMEM)
    return pl.pallas_call(
        compose_kernel,
        out_shape=(
            jax.ShapeDtypeStruct((count, width), jnp.int32),
            jax.ShapeDtypeStruct((1, width), jnp.float32),
        ),
        in_specs=[vmem, vmem, vmem, pl.BlockSpec(memory_space=pltpu.SMEM), vmem],
        out_specs=(vmem, vmem),
        name="compose",
    )(match_one, two, three, own, weights)


def encode(piece):
    top = jnp.max(jnp.abs(piece), axis=0, keepdims=True)
    exponent = jnp.ceil(jnp.log2(jnp.maximum(top, 1e-30)) * STEP)
    factor = jnp.exp2(exponent * (-1.0 / STEP)) * LEVELS
    return jnp.round(piece * factor).astype(jnp.int32).astype(jnp.int16), exponent


def encode_out(total_ref, out_ref, dest, rows):
    held = total_ref.shape[0] // out_ref.shape[0]
    width = total_ref.shape[2]
    exponents = []
    for place in range(held):
        piece = total_ref[dest * held + place]
        coded, exponent = encode(piece)
        out_ref[dest, pl.ds(place * rows, rows), :] = coded
        exponents.append(exponent)
    pad = up(held, 16) - held
    if pad:
        exponents.append(jnp.zeros((pad, width), jnp.float32))
    tail = jnp.concatenate(exponents, axis=0)
    out_ref[dest, pl.ds(held * rows, held + pad), :] = tail.astype(jnp.int32).astype(jnp.int16)


def project_kernel(per_step, halves, rows_ref, cols_ref, slots_ref, table_ref, blocks_ref, *refs):
    outs, totals = refs[:halves], refs[halves:]
    step = pl.program_id(0)
    width = blocks_ref.shape[2]
    part = width // halves

    @pl.when(step == 0)
    def _():
        for total_ref in totals:
            total_ref[...] = jnp.zeros_like(total_ref)

    for place in range(per_step):
        k = step * per_step + place
        left = one_hot(table_ref[pl.ds(rows_ref[k], 1), :], width)
        right = one_hot(table_ref[pl.ds(cols_ref[k], 1), :], width)
        half = jnp.dot(left, blocks_ref[place], preferred_element_type=jnp.float32)
        high = half.astype(jnp.bfloat16)
        low = (half - high.astype(jnp.float32)).astype(jnp.bfloat16)
        both = contract_lanes(
            jnp.concatenate([high, low], axis=1), jnp.concatenate([right, right], axis=1)
        )
        slot = slots_ref[k]
        for h, total_ref in enumerate(totals):
            total_ref[slot] += both[h * part : (h + 1) * part]

    @pl.when(step == pl.num_programs(0) - 1)
    def _():
        for total_ref, out_ref in zip(totals, outs):
            lax.fori_loop(
                0, out_ref.shape[0],
                lambda dest, _: (encode_out(total_ref, out_ref, dest, part), 0)[1], 0)


def coded_rows(held, rows):
    return held * rows + up(held, 16)


def project_sum(blocks, rows, cols, slots, table, count, dests, halves):
    number, width = blocks.shape[:2]
    per_step = number // FINE_STEPS
    part = width // halves
    shape = (dests, coded_rows(count // dests, part), width)
    return pl.pallas_call(
        functools.partial(project_kernel, per_step, halves),
        grid_spec=pltpu.PrefetchScalarGridSpec(
            num_scalar_prefetch=3,
            grid=(FINE_STEPS,),
            in_specs=[
                pl.BlockSpec(table.shape, lambda s, *_: (0, 0)),
                pl.BlockSpec((per_step, width, width), lambda s, *_: (s, 0, 0)),
            ],
            out_specs=[pl.BlockSpec(shape, lambda s, *_: (0, 0, 0))] * halves,
            scratch_shapes=[pltpu.VMEM((count, part, width), jnp.float32)] * halves,
        ),
        out_shape=[jax.ShapeDtypeStruct(shape, jnp.int16)] * halves,
        compiler_params=pltpu.CompilerParams(vmem_limit_bytes=48 * 1024 * 1024),
        name="project_sum",
    )(rows, cols, slots, table, blocks)


def merge_kernel(held, rows, coded, slots_ref, in_ref, out_ref, *scratch):
    total_ref = scratch[0] if coded else out_ref
    source = pl.program_id(0)

    @pl.when(source == 0)
    def _():
        total_ref[...] = jnp.zeros_like(total_ref)

    tail = in_ref[0, pl.ds(held * rows, up(held, 16)), :].astype(jnp.int32).astype(jnp.float32)
    factors = jnp.exp2(tail * (1.0 / STEP)) * (1.0 / LEVELS)
    for place in range(held):
        piece = in_ref[0, pl.ds(place * rows, rows), :].astype(jnp.int32).astype(jnp.float32)
        slot = slots_ref[source * held + place]
        total_ref[slot] += piece * factors[place : place + 1, :]

    if coded:
        @pl.when(source == pl.num_programs(0) - 1)
        def _():
            lax.fori_loop(
                0, out_ref.shape[0],
                lambda dest, _: (encode_out(total_ref, out_ref, dest, rows), 0)[1], 0)


def merge(received, slots, count, rows, dests):
    sources, _, width = received.shape
    held = slots.shape[0] // sources
    if dests:
        shape, kind = (dests, coded_rows(count // dests, rows), width), jnp.int16
        scratch = [pltpu.VMEM((count, rows, width), jnp.float32)]
    else:
        shape, kind, scratch = (count, rows, width), jnp.float32, []
    return pl.pallas_call(
        functools.partial(merge_kernel, held, rows, bool(dests)),
        grid_spec=pltpu.PrefetchScalarGridSpec(
            num_scalar_prefetch=1,
            grid=(sources,),
            in_specs=[pl.BlockSpec((1,) + received.shape[1:], lambda s, *_: (s, 0, 0))],
            out_specs=pl.BlockSpec(shape, lambda s, *_: (0, 0, 0)),
            scratch_shapes=scratch,
        ),
        out_shape=jax.ShapeDtypeStruct(shape, kind),
        compiler_params=pltpu.CompilerParams(vmem_limit_bytes=40 * 1024 * 1024),
        name="merge",
    )(slots, received)


def exchange(array, axis):
    return lax.all_to_all(array, axis, split_axis=0, concat_axis=0, tiled=True)


def per_device(
    blocks, ids_one, ids_two, ids_three, match_one, match_two, match_three,
    target_one, target_two, target_three, vertex_weights,
):
    fine = blocks.shape[0]
    devs, groups = lax.axis_size("dev"), lax.axis_size("grp")
    share, share_two = fine // devs, fine // 2 // devs

    fine_in = exchange(blocks, "dev")
    labels = jnp.concatenate(
        [ids_one[0].reshape(devs, share), ids_one[1].reshape(devs, share),
         target_one.reshape(devs, share), target_two.reshape(devs, share_two)], axis=1
    ).astype(jnp.float32)
    own_sum = jnp.full((devs, 1), jnp.sum(vertex_weights))
    arrived = exchange(jnp.concatenate([labels, own_sum], axis=1), "dev")
    whole = arrived[:, : 3 * share + share_two].astype(jnp.int32)
    group_sum = jnp.sum(arrived[:, -1])
    arrived_three = exchange(
        jnp.concatenate(
            [target_three.reshape(groups, -1).astype(jnp.float32), jnp.full((groups, 1), group_sum)],
            axis=1), "grp")
    total = jnp.sum(arrived_three[:, -1])
    slots_three = arrived_three[:, :-1].astype(jnp.int32).reshape(-1)
    rows = whole[:, :share].reshape(-1)
    cols = whole[:, share : 2 * share].reshape(-1)
    slots = whole[:, 2 * share : 3 * share].reshape(-1)
    slots_two = whole[:, 3 * share :].reshape(-1)

    position = lax.axis_index(("grp", "dev"))
    table, weights_three = compose(match_one, match_two, match_three, vertex_weights, position)
    vertices = lax.axis_size(("grp", "dev")) * weights_three.shape[1]
    rel_weight = weights_three * vertices / total

    part = blocks.shape[1] // HALVES
    pieces = project_sum(fine_in, rows, cols, slots, table, fine // 2, devs, HALVES)
    received = [exchange(piece, "dev") for piece in pieces]
    seconds = [merge(piece, slots_two, fine // 4, part, groups) for piece in received]
    thirds = [exchange(piece, "grp") for piece in seconds]
    finals = [merge(piece, slots_three, fine // 8, part, 0) for piece in thirds]
    return (jnp.concatenate(finals, axis=1), rel_weight)


def solution(mesh):
    whole = P(("grp", "dev"))
    return jax.shard_map(
        per_device,
        mesh=mesh,
        in_specs=(
            P(("grp", "dev"), None, None),
            P(None, ("grp", "dev")),
            P(None, ("grp", "dev")),
            P(None, ("grp", "dev")),
            P(),
            P(),
            P(),
            whole,
            whole,
            whole,
            P(("grp", "dev"), None),
        ),
        out_specs=(P(("grp", "dev"), None, None), P(("grp", "dev"), None)),
        check_vma=False,
    )
```

```python
import functools

import jax
import jax.numpy as jnp
from jax import lax
from jax.experimental import pallas as pl
from jax.experimental.pallas import tpu as pltpu
from jax.sharding import PartitionSpec as P

LEVELS = 32766.0
STEP = 16.0
HALVES = 2


def up(count, unit):
    return -(-count // unit) * unit


def one_hot(indices, width):
    rows = lax.broadcasted_iota(jnp.int32, (width, indices.shape[1]), 0)
    return jnp.where(rows == indices, 1.0, 0.0).astype(jnp.bfloat16)


def contract_lanes(left, right):
    return lax.dot_general(
        left, right, (((1,), (1,)), ((), ())), preferred_element_type=jnp.float32
    )


def compose_kernel(one_ref, two_ref, three_ref, own_ref, weights_ref, table_ref, coarse_ref):
    middle = jnp.take_along_axis(two_ref[...], one_ref[...], axis=1)
    table_ref[...] = jnp.take_along_axis(three_ref[...], middle, axis=1)
    owned, width = weights_ref.shape
    total = jnp.zeros((8, width), jnp.float32)
    for row in range(owned):
        hot = one_hot(table_ref[pl.ds(own_ref[0] + row, 1), :], width)
        value = weights_ref[row : row + 1, :]
        high = value.astype(jnp.bfloat16)
        rest = value - high.astype(jnp.float32)
        middle_part = rest.astype(jnp.bfloat16)
        low = (rest - middle_part.astype(jnp.float32)).astype(jnp.bfloat16)
        parts = jnp.concatenate(
            [high.astype(jnp.float32), middle_part.astype(jnp.float32), low.astype(jnp.float32),
             jnp.zeros((5, width), jnp.float32)], axis=0).astype(jnp.bfloat16)
        total = total + contract_lanes(parts, hot)
    coarse_ref[...] = jnp.sum(total, axis=0, keepdims=True)


def compose(match_one, match_two, match_three, weights, position):
    count, width = match_one.shape
    two = jnp.repeat(match_two, 2, axis=0)
    three = jnp.repeat(match_three, 4, axis=0)
    own = (position * weights.shape[0]).astype(jnp.int32).reshape(1)
    vmem = pl.BlockSpec(memory_space=pltpu.VMEM)
    return pl.pallas_call(
        compose_kernel,
        out_shape=(
            jax.ShapeDtypeStruct((count, width), jnp.int32),
            jax.ShapeDtypeStruct((1, width), jnp.float32),
        ),
        in_specs=[vmem, vmem, vmem, pl.BlockSpec(memory_space=pltpu.SMEM), vmem],
        out_specs=(vmem, vmem),
        name="compose",
    )(match_one, two, three, own, weights)


def encode(piece):
    top = jnp.max(jnp.abs(piece), axis=0, keepdims=True)
    exponent = jnp.ceil(jnp.log2(jnp.maximum(top, 1e-30)) * STEP)
    factor = jnp.exp2(exponent * (-1.0 / STEP)) * LEVELS
    return jnp.round(piece * factor).astype(jnp.int32).astype(jnp.int16), exponent


def partner(place, index, count, back=False):
    if count & (count - 1) == 0:
        return index ^ place
    return lax.rem(index + (count - place if back else place), count)


def pairs(place, count):
    if count & (count - 1) == 0:
        return [(i, i ^ place) for i in range(count)]
    return [(i, (i + place) % count) for i in range(count)]


def encode_out(total_ref, out_ref, base, rows, first):
    width = total_ref.shape[2]
    held = (out_ref.shape[0] - 16) // rows
    exponents = []
    for place in range(held):
        coded, exponent = encode(total_ref[base + place, first : first + rows])
        out_ref[place * rows : (place + 1) * rows, :] = coded
        exponents.append(exponent)
    pad = up(held, 16) - held
    if pad:
        exponents.append(jnp.zeros((pad, width), jnp.float32))
    tail = jnp.concatenate(exponents, axis=0)
    out_ref[held * rows : held * rows + held + pad, :] = tail.astype(jnp.int32).astype(jnp.int16)


def coded_rows(held, rows):
    return held * rows + up(held, 16)


def project_kernel(places, devs, halves, first, me_ref, rows_ref, cols_ref, slots_ref, table_ref, *refs):
    sources, refs = refs[: len(places)], refs[len(places) :]
    total_ref, outs = (refs[0], refs[1:]) if first else (refs[1], refs[2:])
    if first:
        total_ref[...] = jnp.zeros_like(total_ref)
    for place, source_ref in zip(places, sources):
        share, width = source_ref.shape[:2]
        unit = min(4, share)
        base = partner(place, me_ref[0], devs, True) * share

        def body(turn, _):
            for inner in range(unit):
                at = turn * unit + inner
                k = base + at
                left = one_hot(table_ref[pl.ds(rows_ref[k], 1), :], width)
                right = one_hot(table_ref[pl.ds(cols_ref[k], 1), :], width)
                half = jnp.dot(left, source_ref[at], preferred_element_type=jnp.float32)
                high = half.astype(jnp.bfloat16)
                low = (half - high.astype(jnp.float32)).astype(jnp.bfloat16)
                total_ref[slots_ref[k]] += contract_lanes(
                    jnp.concatenate([high, low], axis=1), jnp.concatenate([right, right], axis=1)
                )
            return 0

        lax.fori_loop(0, share // unit, body, 0)
    if halves:
        held = total_ref.shape[0] // devs
        part = total_ref.shape[1] // halves
        for h in range(halves):
            for place in range(devs):
                base = partner(place, me_ref[0], devs) * held
                encode_out(total_ref, outs[h * devs + place], base, part, h * part)


def project_sum(sources, places, total, me, labels, table, count, devs, halves):
    width = table.shape[1]
    first = total is None
    vmem = pl.BlockSpec(memory_space=pltpu.VMEM)
    smem = pl.BlockSpec(memory_space=pltpu.SMEM)
    operands = [me, *labels, table, *sources] + ([] if first else [total])
    out_shape = [jax.ShapeDtypeStruct((count, width, width), jnp.float32)]
    if halves:
        part = width // halves
        shape = (coded_rows(count // devs, part), width)
        out_shape += [jax.ShapeDtypeStruct(shape, jnp.int16)] * (halves * devs)
    alias = {} if first else {len(operands) - 1: 0}
    return pl.pallas_call(
        functools.partial(project_kernel, places, devs, halves, first),
        out_shape=out_shape,
        in_specs=[smem] * 4 + [vmem] * (len(operands) - 4),
        out_specs=[vmem] * len(out_shape),
        input_output_aliases=alias,
        compiler_params=pltpu.CompilerParams(vmem_limit_bytes=24 * 1024 * 1024),
        name="project_sum",
    )(*operands)


def merge_kernel(axis_size, rows, dests, me_ref, slots_ref, *refs):
    sources, refs = refs[:axis_size], refs[axis_size:]
    held = slots_ref.shape[0] // axis_size
    if dests:
        outs, total_ref = refs[1:-1], refs[-1]
    else:
        total_ref = refs[-1]
    total_ref[...] = jnp.zeros_like(total_ref)
    for place, source_ref in enumerate(sources):
        base = partner(place, me_ref[0], axis_size, True) * held
        tail = source_ref[held * rows :, :].astype(jnp.int32).astype(jnp.float32)
        factors = jnp.exp2(tail * (1.0 / STEP)) * (1.0 / LEVELS)
        for at in range(held):
            piece = source_ref[at * rows : (at + 1) * rows, :].astype(jnp.int32).astype(jnp.float32)
            total_ref[slots_ref[base + at]] += piece * factors[at : at + 1, :]
    if dests:
        part = total_ref.shape[0] // dests
        for place in range(dests):
            encode_out(
                total_ref, outs[place], partner(place, refs[0][0], dests) * part, rows, 0)


def merge(received, slots, me, count, rows, dests, group):
    width = received[0].shape[1]
    vmem = pl.BlockSpec(memory_space=pltpu.VMEM)
    smem = pl.BlockSpec(memory_space=pltpu.SMEM)
    if dests:
        shape = (coded_rows(count // dests, rows), width)
        out_shape = [jax.ShapeDtypeStruct(shape, jnp.int16)] * dests
        scratch = [pltpu.VMEM((count, rows, width), jnp.float32)]
    else:
        out_shape = [jax.ShapeDtypeStruct((count, rows, width), jnp.float32)]
        scratch = []
    return pl.pallas_call(
        functools.partial(merge_kernel, len(received), rows, dests),
        out_shape=out_shape,
        in_specs=[smem] * 2 + [vmem] * len(received) + [smem],
        out_specs=[vmem] * len(out_shape),
        scratch_shapes=scratch,
        compiler_params=pltpu.CompilerParams(vmem_limit_bytes=24 * 1024 * 1024),
        name="merge",
    )(me, slots, *received, group)


def swap(pieces, axis, order):
    count = len(pieces)
    out = list(pieces)
    for place in order:
        out[place] = lax.ppermute(pieces[place], axis, pairs(place, count))
    return out


def far_first(count):
    return sorted(range(1, count), key=lambda p: (-bin(p >> 1).count("1"), p & 1, p))


def exchange(array, axis):
    return lax.all_to_all(array, axis, split_axis=0, concat_axis=0, tiled=True)


def per_device(
    blocks, ids_one, ids_two, ids_three, match_one, match_two, match_three,
    target_one, target_two, target_three, vertex_weights,
):
    fine = blocks.shape[0]
    devs, groups = lax.axis_size("dev"), lax.axis_size("grp")
    share, share_two = fine // devs, fine // 2 // devs

    me = lax.axis_index("dev").astype(jnp.int32)
    group = lax.axis_index("grp").astype(jnp.int32)
    order = far_first(devs)
    fine_in = swap(
        [lax.dynamic_slice_in_dim(blocks, partner(p, me, devs) * share, share, 0) for p in range(devs)],
        "dev", order)
    labels = jnp.concatenate(
        [ids_one[0].reshape(devs, share), ids_one[1].reshape(devs, share),
         target_one.reshape(devs, share), target_two.reshape(devs, share_two)], axis=1
    ).astype(jnp.float32)
    own_sum = jnp.full((devs, 1), jnp.sum(vertex_weights))
    arrived = exchange(jnp.concatenate([labels, own_sum], axis=1), "dev")
    whole = arrived[:, : 3 * share + share_two].astype(jnp.int32)
    group_sum = jnp.sum(arrived[:, -1])
    arrived_three = exchange(
        jnp.concatenate(
            [target_three.reshape(groups, -1).astype(jnp.float32), jnp.full((groups, 1), group_sum)],
            axis=1), "grp")
    total = jnp.sum(arrived_three[:, -1])
    slots_three = arrived_three[:, :-1].astype(jnp.int32).reshape(-1)
    rows = whole[:, :share].reshape(-1)
    cols = whole[:, share : 2 * share].reshape(-1)
    slots = whole[:, 2 * share : 3 * share].reshape(-1)
    slots_two = whole[:, 3 * share :].reshape(-1)

    position = lax.axis_index(("grp", "dev"))
    table, weights_three = compose(match_one, match_two, match_three, vertex_weights, position)
    vertices = lax.axis_size(("grp", "dev")) * weights_three.shape[1]
    rel_weight = weights_three * vertices / total

    part = blocks.shape[1] // HALVES
    me, group = me.reshape(1), group.reshape(1)
    turns = [0] + ([1] if devs > 1 else []) + [p for p in order if p > 1]
    bunches = [turns[i : i + 2] for i in range(0, len(turns), 2)]
    sums = None
    for i, bunch in enumerate(bunches):
        last = i == len(bunches) - 1
        outs = project_sum(
            [fine_in[p] for p in bunch], bunch, sums, me, (rows, cols, slots), table, fine // 2,
            devs, HALVES if last else 0)
        sums = outs[0]
    results = []
    for h in range(HALVES):
        received = swap(outs[1 + h * devs : 1 + (h + 1) * devs], "dev", order)
        seconds = merge(received, slots_two, me, fine // 4, part, groups, group)
        thirds = swap(seconds, "grp", far_first(groups))
        results += merge(thirds, slots_three, group, fine // 8, part, 0, group)
    return (jnp.concatenate(results, axis=1), rel_weight)


def solution(mesh):
    whole = P(("grp", "dev"))
    return jax.shard_map(
        per_device,
        mesh=mesh,
        in_specs=(
            P(("grp", "dev"), None, None),
            P(None, ("grp", "dev")),
            P(None, ("grp", "dev")),
            P(None, ("grp", "dev")),
            P(),
            P(),
            P(),
            whole,
            whole,
            whole,
            P(("grp", "dev"), None),
        ),
        out_specs=(P(("grp", "dev"), None, None), P(("grp", "dev"), None)),
        check_vma=False,
    )
```

```python
import functools

import jax
import jax.numpy as jnp
from jax import lax
from jax.experimental import pallas as pl
from jax.experimental.pallas import tpu as pltpu
from jax.sharding import PartitionSpec as P


LEVELS = 32766.0
STEP = 16.0
HALVES = 2


def up(count, unit):
    return -(-count // unit) * unit


def one_hot(indices, width):
    rows = lax.broadcasted_iota(jnp.int32, (width, indices.shape[1]), 0)
    return jnp.where(rows == indices, 1.0, 0.0).astype(jnp.bfloat16)


def contract_lanes(left, right):
    return lax.dot_general(
        left, right, (((1,), (1,)), ((), ())), preferred_element_type=jnp.float32
    )


def compose_kernel(one_ref, two_ref, three_ref, own_ref, weights_ref, table_ref, coarse_ref):
    middle = jnp.take_along_axis(two_ref[...], one_ref[...], axis=1)
    table_ref[...] = jnp.take_along_axis(three_ref[...], middle, axis=1)
    owned, width = weights_ref.shape
    total = jnp.zeros((8, width), jnp.float32)
    for row in range(owned):
        hot = one_hot(table_ref[pl.ds(own_ref[0] + row, 1), :], width)
        value = weights_ref[row : row + 1, :]
        high = value.astype(jnp.bfloat16)
        rest = value - high.astype(jnp.float32)
        middle_part = rest.astype(jnp.bfloat16)
        low = (rest - middle_part.astype(jnp.float32)).astype(jnp.bfloat16)
        parts = jnp.concatenate(
            [high.astype(jnp.float32), middle_part.astype(jnp.float32), low.astype(jnp.float32),
             jnp.zeros((5, width), jnp.float32)], axis=0).astype(jnp.bfloat16)
        total = total + contract_lanes(parts, hot)
    coarse_ref[...] = jnp.sum(total, axis=0, keepdims=True)


def compose(match_one, match_two, match_three, weights, position):
    count, width = match_one.shape
    two = jnp.repeat(match_two, 2, axis=0)
    three = jnp.repeat(match_three, 4, axis=0)
    own = (position * weights.shape[0]).astype(jnp.int32).reshape(1)
    vmem = pl.BlockSpec(memory_space=pltpu.VMEM)
    return pl.pallas_call(
        compose_kernel,
        out_shape=(
            jax.ShapeDtypeStruct((count, width), jnp.int32),
            jax.ShapeDtypeStruct((1, width), jnp.float32),
        ),
        in_specs=[vmem, vmem, vmem, pl.BlockSpec(memory_space=pltpu.SMEM), vmem],
        out_specs=(vmem, vmem),
        name="compose",
    )(match_one, two, three, own, weights)


def encode(piece):
    top = jnp.max(jnp.abs(piece), axis=0, keepdims=True)
    exponent = jnp.ceil(jnp.log2(jnp.maximum(top, 1e-30)) * STEP)
    factor = jnp.exp2(exponent * (-1.0 / STEP)) * LEVELS
    return jnp.round(piece * factor).astype(jnp.int32).astype(jnp.int16), exponent


def partner(place, index, count, back=False):
    if count & (count - 1) == 0:
        return index ^ place
    return lax.rem(index + (count - place if back else place), count)


def pairs(place, count):
    if count & (count - 1) == 0:
        return [(i, i ^ place) for i in range(count)]
    return [(i, (i + place) % count) for i in range(count)]


def encode_out(total_ref, out_ref, base, rows, first):
    width = total_ref.shape[2]
    held = (out_ref.shape[0] - 16) // rows
    exponents = []
    for place in range(held):
        coded, exponent = encode(total_ref[base + place, first : first + rows])
        out_ref[place * rows : (place + 1) * rows, :] = coded
        exponents.append(exponent)
    pad = up(held, 16) - held
    if pad:
        exponents.append(jnp.zeros((pad, width), jnp.float32))
    tail = jnp.concatenate(exponents, axis=0)
    out_ref[held * rows : held * rows + held + pad, :] = tail.astype(jnp.int32).astype(jnp.int16)


def coded_rows(held, rows):
    return held * rows + up(held, 16)


def project_kernel(places, devs, halves, first, me_ref, rows_ref, cols_ref, slots_ref, table_ref, *refs):
    sources, refs = refs[: len(places)], refs[len(places) :]
    total_ref, outs = (refs[0], refs[1:]) if first else (refs[1], refs[2:])
    if first:
        total_ref[...] = jnp.zeros_like(total_ref)
    for place, source_ref in zip(places, sources):
        share, width = source_ref.shape[:2]
        unit = min(4, share)
        base = partner(place, me_ref[0], devs, True) * share

        def body(turn, _):
            found = []
            for inner in range(unit):
                at = turn * unit + inner
                k = base + at
                left = one_hot(table_ref[pl.ds(rows_ref[k], 1), :], width)
                right = one_hot(table_ref[pl.ds(cols_ref[k], 1), :], width)
                half = jnp.dot(left, source_ref[at], preferred_element_type=jnp.float32)
                high = half.astype(jnp.bfloat16)
                low = (half - high.astype(jnp.float32)).astype(jnp.bfloat16)
                found.append((k, contract_lanes(
                    jnp.concatenate([high, low], axis=1), jnp.concatenate([right, right], axis=1)
                )))
            for k, both in found:
                total_ref[slots_ref[k]] += both
            return 0

        lax.fori_loop(0, share // unit, body, 0)
    if halves:
        code_half(me_ref[0], devs, halves, 0, total_ref, outs)


def code_half(me, devs, halves, h, total_ref, outs):
    held = total_ref.shape[0] // devs
    part = total_ref.shape[1] // halves
    for place in range(devs):
        encode_out(total_ref, outs[place], partner(place, me, devs) * held, part, h * part)


def code_kernel(devs, halves, h, me_ref, total_ref, *outs):
    code_half(me_ref[0], devs, halves, h, total_ref, outs)


def code(total, me, devs, halves, h):
    count, width = total.shape[:2]
    part = width // halves
    vmem = pl.BlockSpec(memory_space=pltpu.VMEM)
    shape = (coded_rows(count // devs, part), width)
    return pl.pallas_call(
        functools.partial(code_kernel, devs, halves, h),
        out_shape=[jax.ShapeDtypeStruct(shape, jnp.int16)] * devs,
        in_specs=[pl.BlockSpec(memory_space=pltpu.SMEM), vmem],
        out_specs=[vmem] * devs,
        compiler_params=pltpu.CompilerParams(vmem_limit_bytes=24 * 1024 * 1024),
        name="code",
    )(me, total)


def project_sum(sources, places, total, me, labels, table, count, devs, halves):
    width = table.shape[1]
    first = total is None
    vmem = pl.BlockSpec(memory_space=pltpu.VMEM)
    smem = pl.BlockSpec(memory_space=pltpu.SMEM)
    operands = [me, *labels, table, *sources] + ([] if first else [total])
    out_shape = [jax.ShapeDtypeStruct((count, width, width), jnp.float32)]
    if halves:
        part = width // halves
        shape = (coded_rows(count // devs, part), width)
        out_shape += [jax.ShapeDtypeStruct(shape, jnp.int16)] * devs
    alias = {} if first else {len(operands) - 1: 0}
    return pl.pallas_call(
        functools.partial(project_kernel, places, devs, halves, first),
        out_shape=out_shape,
        in_specs=[smem] * 4 + [vmem] * (len(operands) - 4),
        out_specs=[vmem] * len(out_shape),
        input_output_aliases=alias,
        compiler_params=pltpu.CompilerParams(vmem_limit_bytes=24 * 1024 * 1024),
        name="project_sum",
    )(*operands)


def merge_kernel(axis_size, rows, dests, me_ref, slots_ref, *refs):
    sources, refs = refs[:axis_size], refs[axis_size:]
    held = slots_ref.shape[0] // axis_size
    outs, total_ref = refs[1:-1], refs[-1]
    total_ref[...] = jnp.zeros_like(total_ref)
    for place, source_ref in enumerate(sources):
        base = partner(place, me_ref[0], axis_size, True) * held
        tail = source_ref[held * rows :, :].astype(jnp.int32).astype(jnp.float32)
        factors = jnp.exp2(tail * (1.0 / STEP)) * (1.0 / LEVELS)
        for at in range(held):
            piece = source_ref[at * rows : (at + 1) * rows, :].astype(jnp.int32).astype(jnp.float32)
            total_ref[slots_ref[base + at]] += piece * factors[at : at + 1, :]
    if dests:
        part = total_ref.shape[0] // dests
        for place in range(dests):
            encode_out(
                total_ref, outs[place], partner(place, refs[0][0], dests) * part, rows, 0)


def merge(received, slots, me, count, rows, dests, group):
    width = received[0].shape[1]
    vmem = pl.BlockSpec(memory_space=pltpu.VMEM)
    smem = pl.BlockSpec(memory_space=pltpu.SMEM)
    shape = (coded_rows(count // dests, rows), width)
    return pl.pallas_call(
        functools.partial(merge_kernel, len(received), rows, dests),
        out_shape=[jax.ShapeDtypeStruct(shape, jnp.int16)] * dests,
        in_specs=[smem] * 2 + [vmem] * len(received) + [smem],
        out_specs=[vmem] * dests,
        scratch_shapes=[pltpu.VMEM((count, rows, width), jnp.float32)],
        compiler_params=pltpu.CompilerParams(vmem_limit_bytes=24 * 1024 * 1024),
        name="merge",
    )(me, slots, *received, group)


def merge_last(received, slots, me, count, rows, h, result):
    width = received[0].shape[1]
    operands = [me, slots, *received] + ([] if result is None else [result])
    specs = [pl.BlockSpec(memory_space=pltpu.SMEM)] * 2
    specs += [pl.BlockSpec(piece.shape, lambda _: (0, 0)) for piece in received]
    if result is not None:
        specs.append(pl.BlockSpec(memory_space=pl.ANY))
    return pl.pallas_call(
        functools.partial(merge_kernel, len(received), rows, 0),
        out_shape=jax.ShapeDtypeStruct((count, width, width), jnp.float32),
        grid=(1,),
        in_specs=specs,
        out_specs=pl.BlockSpec((count, rows, width), lambda _: (0, h, 0)),
        input_output_aliases={} if result is None else {len(operands) - 1: 0},
        compiler_params=pltpu.CompilerParams(vmem_limit_bytes=24 * 1024 * 1024),
        name="merge_last",
    )(*operands)


def swap(pieces, axis, order):
    count = len(pieces)
    out = list(pieces)
    for place in order:
        out[place] = lax.ppermute(pieces[place], axis, pairs(place, count))
    return out


def far_first(count):
    return sorted(range(1, count), key=lambda p: (-bin(p >> 1).count("1"), p & 1, p))


def exchange(array, axis):
    return lax.all_to_all(array, axis, split_axis=0, concat_axis=0, tiled=True)


def per_device(
    blocks, ids_one, ids_two, ids_three, match_one, match_two, match_three,
    target_one, target_two, target_three, vertex_weights,
):
    fine = blocks.shape[0]
    devs, groups = lax.axis_size("dev"), lax.axis_size("grp")
    share, share_two = fine // devs, fine // 2 // devs

    me = lax.axis_index("dev").astype(jnp.int32)
    group = lax.axis_index("grp").astype(jnp.int32)
    order = far_first(devs)
    fine_in, source = [None] * devs, blocks
    for step in (order[:2], order[2:4], order[4:] + [0]):
        parts = [
            lax.dynamic_slice_in_dim(source, partner(p, me, devs) * share, share, 0) for p in step]
        source, *parts = lax.optimization_barrier((source, *parts))
        for p, part in zip(step, parts):
            fine_in[p] = lax.ppermute(part, "dev", pairs(p, devs)) if p else part
    (ids_one, target_one, target_two, target_three, vertex_weights, fine_in[0],
     match_one, match_two, match_three) = lax.optimization_barrier(
        (ids_one, target_one, target_two, target_three, vertex_weights, fine_in[0],
         match_one, match_two, match_three))
    labels = jnp.concatenate(
    [ids_one[0].reshape(devs, share), ids_one[1].reshape(devs, share),
     target_one.reshape(devs, share), target_two.reshape(devs, share_two)], axis=1
    ).astype(jnp.float32)
    own_sum = jnp.full((devs, 1), jnp.sum(vertex_weights))
    labels = jnp.concatenate([labels, own_sum], axis=1)
    arrived = exchange(labels, "dev")
    whole = arrived[:, : 3 * share + share_two].astype(jnp.int32)
    group_sum = jnp.sum(arrived[:, -1])
    arrived_three = exchange(
        jnp.concatenate(
            [target_three.reshape(groups, -1).astype(jnp.float32), jnp.full((groups, 1), group_sum)],
            axis=1), "grp")
    total = jnp.sum(arrived_three[:, -1])
    slots_three = arrived_three[:, :-1].astype(jnp.int32).reshape(-1)
    rows = whole[:, :share].reshape(-1)
    cols = whole[:, share : 2 * share].reshape(-1)
    slots = whole[:, 2 * share : 3 * share].reshape(-1)
    slots_two = whole[:, 3 * share :].reshape(-1)

    position = lax.axis_index(("grp", "dev"))
    table, weights_three = compose(match_one, match_two, match_three, vertex_weights, position)
    vertices = lax.axis_size(("grp", "dev")) * weights_three.shape[1]
    rel_weight = weights_three * vertices / total

    part = blocks.shape[1] // HALVES
    me, group = me.reshape(1), group.reshape(1)
    turns = [0] + ([1] if devs > 1 else []) + [p for p in order if p > 1]
    bunches = [turns[i : i + 2] for i in range(0, len(turns), 2)]
    sums = None
    for i, bunch in enumerate(bunches):
        last = i == len(bunches) - 1
        outs = project_sum(
            [fine_in[p] for p in bunch], bunch, sums, me, (rows, cols, slots), table, fine // 2,
            devs, HALVES if last else 0)
        sums = outs[0]
    result = None
    for h in range(HALVES):
        coded = outs[1:] if h == 0 else code(sums, me, devs, HALVES, h)
        received = swap(coded, "dev", order)
        seconds = merge(received, slots_two, me, fine // 4, part, groups, group)
        thirds = swap(seconds, "grp", far_first(groups))
        result = merge_last(thirds, slots_three, group, fine // 8, part, h, result)
    return (result, rel_weight)


def solution(mesh):
    whole = P(("grp", "dev"))
    return jax.shard_map(
        per_device,
        mesh=mesh,
        in_specs=(
            P(("grp", "dev"), None, None),
            P(None, ("grp", "dev")),
            P(None, ("grp", "dev")),
            P(None, ("grp", "dev")),
            P(),
            P(),
            P(),
            whole,
            whole,
            whole,
            P(("grp", "dev"), None),
        ),
        out_specs=(P(("grp", "dev"), None, None), P(("grp", "dev"), None)),
        check_vma=False,
    )
```
